32 devices in a mesh: blk: 16 (over z, x, core), cat: 2 (over y).
Axes of the slice: x: 2, y: 2, z: 4, core: 2. Of those that a mesh axis runs over, the one named last changes fastest.
Arguments:
- item_content: bfloat16 [32768, 512], P('blk', 'cat'), may hold values from -6 to 6
- projection: bfloat16 [512, 256], replicated, may hold values from -0.06591797 to 0.06591797
- send_order: int32 [32, 1024], P(('blk', 'cat')), may hold values from 0 to 1023, each once within a row
- user_factors: float32 [16384, 256], P(('blk', 'cat')), may hold values from -1.5 to 1.5
- ratings: int32 [16384, 4, 1024], P(('blk', 'cat')), may hold values from 0 to 5, as said below
Outputs:
- users_out: float32 [16384, 256], P(('blk', 'cat'))
- items_out: float32 [32768, 256], P(('blk', 'cat'))
The draws below stay inside these ranges and needn't reach their ends.
Inputs may be any that keep to these rules, and one draw needn't show every extreme that they name: `send_order`: each row is a permutation of 0 .. 1023. `ratings`: 0 means no rating, 1 to 5 a rating.
All inputs are finite; a program needn't handle non-finite values.
Results may differ from the reference program's by a relative error of at most 0.0003.
Values may be sent and summed in bfloat16 or wider, within the bound.
A program may use at most 64 MiB of HBM per device.

```python
import jax
import jax.numpy as jnp
from jax import lax

R = 256
C = 512
U_DEV = 512
ITEM_DEV = 1024
ROUNDS = 4
USERS = 16384
ITEMS = 32768
N_BLK = 16
N_CAT = 2
DEVICES = 32


def draw_ratings(key, part):
    shape = (USERS, ROUNDS, ITEM_DEV)
    levels = jax.random.randint(jax.random.fold_in(key, 11), shape, 1, 6)
    present = jax.random.randint(jax.random.fold_in(key, 12), shape, 0, 3)
    return jnp.where(present == 0, levels, 0).astype(jnp.int32)


def block_scale(rng, shape, cuts, smallest, largest):
    gain, own = 1.0, jax.random.fold_in(rng, 6)
    for axis_at, blocks in cuts:
        steps = jnp.exp(jax.random.uniform(jax.random.fold_in(own, axis_at), (blocks,), jnp.float32, smallest / len(cuts), largest / len(cuts)))
        gain = gain * jnp.repeat(steps, shape[axis_at] // blocks).reshape([-1 if axis == axis_at else 1 for axis in range(len(shape))])
    return gain


def noise(key, shape, width, bound, cuts=(), held_as=jnp.bfloat16):
    gain = block_scale(key, shape, cuts, -0.22, 0.18) if cuts else 1.0
    drawn = jax.random.normal(key, shape, jnp.float32) * width * gain
    return jnp.minimum(jnp.maximum(drawn, -bound), bound).astype(held_as)


def setup_inputs(seed: int = 0) -> dict:
    keys = jax.random.split(jax.random.key(seed), 6)
    item_content = noise(keys[0], (ITEMS, C), 1.0, 6.0, ((0, 16), (1, 2)))
    projection = noise(keys[1], (C, R), 0.011, 0.06591797)
    send_order = jax.vmap(lambda own: jax.random.permutation(own, ITEM_DEV))(jax.random.split(keys[2], DEVICES)).reshape((DEVICES, ITEM_DEV)).astype(jnp.int32)
    user_factors = noise(keys[3], (USERS, R), 0.25, 1.5, ((0, 32),), jnp.float32)
    ratings = draw_ratings(jax.random.fold_in(keys[5], 71), 0)
    return dict(item_content=item_content, projection=projection, send_order=send_order, user_factors=user_factors, ratings=ratings)


learn_rate = 0.004
shrink = 0.05


def reference(item_content, projection, send_order, user_factors, ratings):
    projected = jnp.dot(item_content, projection, preferred_element_type=jnp.float32)
    blocks = projected.reshape(N_BLK, N_CAT, ITEM_DEV, R)
    orders = send_order.reshape(N_BLK, N_CAT, ITEM_DEV)
    dealt = jnp.take_along_axis(blocks, orders[..., None], axis=2)
    share = ITEM_DEV // N_BLK
    items = dealt.reshape(N_BLK, N_CAT, N_BLK, share, R).transpose(2, 1, 0, 3, 4).reshape(N_BLK, N_CAT, ITEM_DEV, R)
    users = user_factors.reshape(N_BLK, N_CAT, U_DEV, R)
    values_all = ratings.reshape(N_BLK, N_CAT, U_DEV, ROUNDS, ITEM_DEV)
    for round_index in range(ROUNDS):
        if round_index > 0:
            items = jnp.roll(items, 1, axis=0)
        values = values_all[:, :, :, round_index, :].astype(jnp.float32)
        masks = jnp.where(values > 0, jnp.float32(1.0), jnp.float32(0.0))
        guess = jnp.einsum("bcur,bcir->bcui", users, items, precision=lax.Precision.HIGHEST)
        errors = masks * (values - guess)
        user_grad = jnp.einsum("bcui,bcir->bcur", errors, items, precision=lax.Precision.HIGHEST)
        item_grad = jnp.einsum("bcui,bcur->bcir", errors, users, precision=lax.Precision.HIGHEST)
        users, items = (users + learn_rate * (user_grad - shrink * users),
                        items + learn_rate * (item_grad - shrink * items))
    return users.reshape(USERS, R), items.reshape(ITEMS, R)
```

```python
import functools
import jax
import jax.numpy as jnp
from jax import lax
from jax.experimental import pallas as pl
from jax.experimental.pallas import tpu as pltpu
from jax.sharding import PartitionSpec as P

learn_rate = 0.004
shrink = 0.05
LEVELS = 32000.0
STEPS = 20.0
EXTRA = 16
CHUNK = 256
PARTS = 2


def split(value):
    high = value.astype(jnp.bfloat16)
    return high, (value - high.astype(jnp.float32)).astype(jnp.bfloat16)


def product(left, right, dims):
    def one(a, b):
        return lax.dot_general(a, b, (dims, ((), ())), preferred_element_type=jnp.float32)

    return one(left[0], right[0]) + (one(left[0], right[1]) + one(left[1], right[0]))


def code_of(largest):
    return jnp.ceil(jnp.log(jnp.maximum(largest, 1e-30)) * STEPS)


def step_of(code):
    return jnp.exp(code * (1.0 / STEPS)) * (1.0 / LEVELS)


def coded(value, step):
    return jnp.floor(value * (1.0 / step) + 0.5).astype(jnp.int32).astype(jnp.int16)


def unpack_kernel(in_ref, *out_refs):
    for t, out_ref in enumerate(out_refs):
        out_ref[...] = in_ref[:, t, :].astype(jnp.float32).astype(jnp.bfloat16)


def unpack(ratings):
    users, rounds, items = ratings.shape
    block = min(64, users)
    return pl.pallas_call(
        unpack_kernel,
        grid=(users // block,),
        in_specs=[pl.BlockSpec((block, rounds, items), lambda i: (i, 0, 0))],
        out_specs=[pl.BlockSpec((block, items), lambda i: (i, 0))] * rounds,
        out_shape=[jax.ShapeDtypeStruct((users, items), jnp.bfloat16)] * rounds,
        cost_estimate=pl.CostEstimate(
            flops=1000 * ratings.size, bytes_accessed=6 * ratings.size, transcendentals=0
        ),
        name="unpack",
    )(ratings)


def round_kernel(
    packed_in, packed_out, first, last, users_ref, items_ref, values_ref, grad_ref, users_out, items_out
):
    items, rank = values_ref.shape[1], users_ref.shape[1]
    users = users_ref[...]
    user_parts = split(users)
    chunk = min(CHUNK, items)
    user_grad = jnp.zeros(users.shape, jnp.float32) if first else grad_ref[...]
    if packed_in:
        steps_in = step_of(items_ref[items:, :].astype(jnp.int32).astype(jnp.float32))
    if packed_out:
        row = lax.broadcasted_iota(jnp.int32, (EXTRA, rank), 0)
        codes = jnp.zeros((EXTRA, rank), jnp.float32)
    for n in range(items // chunk):
        at = pl.ds(n * chunk, chunk)
        old = items_ref[at, :]
        if packed_in:
            old = old.astype(jnp.int32).astype(jnp.float32) * steps_in[n : n + 1, :]
        old_parts = split(old)
        guess = product(user_parts, old_parts, ((1,), (1,)))
        values = values_ref[:, at].astype(jnp.float32)
        errors = jnp.where(values > 0.0, values - guess, 0.0)
        error_parts = split(errors)
        item_grad = product(error_parts, user_parts, ((0,), (0,)))
        new = old + learn_rate * (item_grad - shrink * old)
        if packed_out:
            code = code_of(jnp.max(jnp.abs(new), axis=0, keepdims=True))
            codes = jnp.where(row == n, code, codes)
            items_out[at, :] = coded(new, step_of(code))
        else:
            items_out[at, :] = new
        user_grad += product(error_parts, old_parts, ((1,), (0,)))
    if packed_out:
        items_out[pl.ds(items, EXTRA), :] = codes.astype(jnp.int32).astype(jnp.int16)
    if last:
        user_grad = users + learn_rate * (user_grad - shrink * users)
    users_out[...] = user_grad


def update(users, items, values, grad, part, packed_in, packed_out):
    n_users, rank = users.shape
    n_items = values.shape[1] // PARTS
    whole = lambda shape: pl.BlockSpec(shape, lambda i: (0, 0))
    out_items = (
        jax.ShapeDtypeStruct((n_items + EXTRA, rank), jnp.int16)
        if packed_out
        else jax.ShapeDtypeStruct((n_items, rank), jnp.float32)
    )
    return pl.pallas_call(
        functools.partial(round_kernel, packed_in, packed_out, part == 0, part == PARTS - 1),
        grid=(1,),
        in_specs=[
            whole(users.shape),
            whole(items.shape),
            pl.BlockSpec((n_users, n_items), lambda i: (0, part)),
            whole(users.shape),
        ],
        out_specs=[whole(users.shape), whole(out_items.shape)],
        out_shape=[jax.ShapeDtypeStruct(users.shape, jnp.float32), out_items],
        cost_estimate=pl.CostEstimate(
            flops=18 * n_users * n_items * rank, bytes_accessed=5 << 20, transcendentals=0
        ),
        compiler_params=pltpu.CompilerParams(vmem_limit_bytes=48 << 20),
        name="sgd_round",
    )(users, items, values, grad)


def body(item_content, projection, send_order, user_factors, ratings):
    size = lax.axis_size("blk")
    rounds = ratings.shape[1]
    own_rows = lax.all_to_all(item_content, "cat", split_axis=0, concat_axis=1, tiled=True)
    values = unpack(ratings)
    owned = jnp.dot(own_rows, projection, preferred_element_type=jnp.float32)
    ordered = owned.at[send_order[0]].get(mode="promise_in_bounds")
    dealt = ordered.reshape(size, -1, ordered.shape[1])
    share = dealt.shape[1]
    code = code_of(jnp.max(jnp.abs(dealt), axis=1, keepdims=True))
    sent = jnp.concatenate(
        [coded(dealt, step_of(code)), code.astype(jnp.int32).astype(jnp.int16)], axis=1
    )
    got = lax.all_to_all(sent, "blk", split_axis=0, concat_axis=0, tiled=True)
    got = got.astype(jnp.int32).astype(jnp.float32)
    items = (got[:, :share] * step_of(got[:, share:])).reshape(owned.shape)
    users = user_factors
    ring = [(i, (i + 1) % size) for i in range(size)]
    parts = jnp.split(items, PARTS)
    for t in range(rounds):
        grad = users
        sent = []
        for part in range(PARTS):
            grad, moved = update(
                users, parts[part], values[t], grad, part, t > 0, t < rounds - 1
            )
            sent.append(lax.ppermute(moved, "blk", ring) if t < rounds - 1 else moved)
        users, parts = grad, sent
    return (users, jnp.concatenate(parts))


def solution(mesh):
    placed = (
        P("blk", "cat"),
        P(),
        P(("blk", "cat"), None),
        P(("blk", "cat"), None),
        P(("blk", "cat"), None, None),
    )
    return jax.shard_map(
        body,
        mesh=mesh,
        in_specs=placed,
        out_specs=(P(("blk", "cat"), None), P(("blk", "cat"), None)),
        check_vma=False,
    )
```

```python
import functools
import jax
import jax.numpy as jnp
from jax import lax
from jax.experimental import pallas as pl
from jax.experimental.pallas import tpu as pltpu
from jax.sharding import PartitionSpec as P

learn_rate = 0.004
shrink = 0.05
LEVELS = 32000.0
STEPS = 20.0
EXTRA = 16
CHUNK = 256
PARTS = 2


def split(value):
    high = value.astype(jnp.bfloat16)
    return high, (value - high.astype(jnp.float32)).astype(jnp.bfloat16)


def product(left, right, dims):
    def one(a, b):
        return lax.dot_general(a, b, (dims, ((), ())), preferred_element_type=jnp.float32)

    return one(left[0], right[0]) + (one(left[0], right[1]) + one(left[1], right[0]))


def code_of(largest):
    return jnp.ceil(jnp.log(jnp.maximum(largest, 1e-30)) * STEPS)


def step_of(code):
    return jnp.exp(code * (1.0 / STEPS)) * (1.0 / LEVELS)


def coded(value, step):
    return jnp.floor(value * (1.0 / step) + 0.5).astype(jnp.int32).astype(jnp.int16)


def unpack_kernel(in_ref, *out_refs):
    for t, out_ref in enumerate(out_refs):
        out_ref[...] = in_ref[:, t, :].astype(jnp.float32).astype(jnp.bfloat16)


def unpack(ratings):
    users, rounds, items = ratings.shape
    block = min(64, users)
    return pl.pallas_call(
        unpack_kernel,
        grid=(users // block,),
        in_specs=[pl.BlockSpec((block, rounds, items), lambda i: (i, 0, 0))],
        out_specs=[pl.BlockSpec((block, items), lambda i: (i, 0))] * rounds,
        out_shape=[jax.ShapeDtypeStruct((users, items), jnp.bfloat16)] * rounds,
        cost_estimate=pl.CostEstimate(
            flops=1000 * ratings.size, bytes_accessed=6 * ratings.size, transcendentals=0
        ),
        name="unpack",
    )(ratings)


def round_kernel(
    packed_in, packed_out, first, last, users_ref, items_ref, values_ref, grad_ref, users_out, items_out
):
    items, rank = values_ref.shape[1], users_ref.shape[1]
    users = users_ref[...]
    user_parts = split(users)
    chunk = min(CHUNK, items)
    user_grad = jnp.zeros(users.shape, jnp.float32) if first else grad_ref[...]
    if packed_in:
        steps_in = step_of(items_ref[items:, :].astype(jnp.int32).astype(jnp.float32))
    if packed_out:
        row = lax.broadcasted_iota(jnp.int32, (EXTRA, rank), 0)
        codes = jnp.zeros((EXTRA, rank), jnp.float32)
    for n in range(items // chunk):
        at = pl.ds(n * chunk, chunk)
        old = items_ref[at, :]
        if packed_in:
            old = old.astype(jnp.int32).astype(jnp.float32) * steps_in[n : n + 1, :]
        old_parts = split(old)
        guess = product(user_parts, old_parts, ((1,), (1,)))
        values = values_ref[:, at].astype(jnp.float32)
        errors = jnp.where(values > 0.0, values - guess, 0.0)
        error_parts = split(errors)
        item_grad = product(error_parts, user_parts, ((0,), (0,)))
        new = old + learn_rate * (item_grad - shrink * old)
        if packed_out:
            code = code_of(jnp.max(jnp.abs(new), axis=0, keepdims=True))
            codes = jnp.where(row == n, code, codes)
            items_out[at, :] = coded(new, step_of(code))
        else:
            items_out[at, :] = new
        user_grad += product(error_parts, old_parts, ((1,), (0,)))
    if packed_out:
        items_out[pl.ds(items, EXTRA), :] = codes.astype(jnp.int32).astype(jnp.int16)
    if last:
        user_grad = users + learn_rate * (user_grad - shrink * users)
    users_out[...] = user_grad


def update(users, items, values, grad, part, packed_in, packed_out):
    n_users, rank = users.shape
    n_items = values.shape[1] // PARTS
    whole = lambda shape: pl.BlockSpec(shape, lambda i: (0, 0))
    out_items = (
        jax.ShapeDtypeStruct((n_items + EXTRA, rank), jnp.int16)
        if packed_out
        else jax.ShapeDtypeStruct((n_items, rank), jnp.float32)
    )
    return pl.pallas_call(
        functools.partial(round_kernel, packed_in, packed_out, part == 0, part == PARTS - 1),
        grid=(1,),
        in_specs=[
            whole(users.shape),
            whole(items.shape),
            pl.BlockSpec((n_users, n_items), lambda i: (0, part)),
            whole(users.shape),
        ],
        out_specs=[whole(users.shape), whole(out_items.shape)],
        out_shape=[jax.ShapeDtypeStruct(users.shape, jnp.float32), out_items],
        cost_estimate=pl.CostEstimate(
            flops=18 * n_users * n_items * rank, bytes_accessed=5 << 20, transcendentals=0
        ),
        compiler_params=pltpu.CompilerParams(vmem_limit_bytes=48 << 20),
        name="sgd_round",
    )(users, items, values, grad)


def project(item_content, projection):
    def dot(rows, weights):
        return jnp.dot(rows, weights, preferred_element_type=jnp.float32)

    if lax.axis_size("cat") != 2:
        rows = lax.all_to_all(item_content, "cat", split_axis=0, concat_axis=1, tiled=True)
        return dot(rows, projection)
    me = lax.axis_index("cat")
    rows, width = item_content.shape[0] // 2, item_content.shape[1]
    other = 1 - me
    theirs = lax.dynamic_slice_in_dim(item_content, other * rows, rows)
    got = lax.ppermute(theirs, "cat", [(0, 1), (1, 0)])
    mine = lax.dynamic_slice_in_dim(item_content, me * rows, rows)
    near = dot(mine, lax.dynamic_slice_in_dim(projection, me * width, width))
    return near + dot(got, lax.dynamic_slice_in_dim(projection, other * width, width))


def body(item_content, projection, send_order, user_factors, ratings):
    size = lax.axis_size("blk")
    rounds = ratings.shape[1]
    values = unpack(ratings)
    owned = project(item_content, projection)
    ordered = owned.at[send_order[0]].get(mode="promise_in_bounds")
    dealt = ordered.reshape(size, -1, ordered.shape[1])
    share = dealt.shape[1]
    code = code_of(jnp.max(jnp.abs(dealt), axis=1, keepdims=True))
    sent = jnp.concatenate(
        [coded(dealt, step_of(code)), code.astype(jnp.int32).astype(jnp.int16)], axis=1
    )
    got = lax.all_to_all(sent, "blk", split_axis=0, concat_axis=0, tiled=True)
    got = got.astype(jnp.int32).astype(jnp.float32)
    items = (got[:, :share] * step_of(got[:, share:])).reshape(owned.shape)
    users = user_factors
    ring = [(i, (i + 1) % size) for i in range(size)]
    parts = jnp.split(items, PARTS)
    for t in range(rounds):
        grad = users
        sent = []
        for part in range(PARTS):
            grad, moved = update(
                users, parts[part], values[t], grad, part, t > 0, t < rounds - 1
            )
            sent.append(lax.ppermute(moved, "blk", ring) if t < rounds - 1 else moved)
        users, parts = grad, sent
    return (users, jnp.concatenate(parts))


def solution(mesh):
    placed = (
        P("blk", "cat"),
        P(),
        P(("blk", "cat"), None),
        P(("blk", "cat"), None),
        P(("blk", "cat"), None, None),
    )
    return jax.shard_map(
        body,
        mesh=mesh,
        in_specs=placed,
        out_specs=(P(("blk", "cat"), None), P(("blk", "cat"), None)),
        check_vma=False,
    )
```
